256 devices in a mesh: row: 16 (over x, z_hi), col: 16 (over y, z_lo, core).
Axes of the slice: x: 4, y: 4, z: 8 (z_hi: 4, z_lo: 2; z = z_hi * 2 + z_lo), core: 2. Of those that a mesh axis runs over, the one named last changes fastest.
Arguments:
- tokens: bfloat16 [2048, 8192], P('col', 'row'), may hold values from -6 to 6
- grad_out: bfloat16 [2048, 8192], P('col', 'row'), may hold values from -2 to 2
- gate: bfloat16 [2048, 14336], P('row', 'col'), may hold values from -6 to 6
- up: bfloat16 [2048, 14336], P('row', 'col'), may hold values from -6 to 6
- gate_weight: bfloat16 [8192, 14336], P('row', 'col'), may hold values from -0.0625 to 0.0625
- up_weight: bfloat16 [8192, 14336], P('row', 'col'), may hold values from -0.0625 to 0.0625
- down_weight: bfloat16 [8192, 14336], P('row', 'col'), may hold values from -0.046875 to 0.046875
Outputs:
- grad_tokens: bfloat16 [2048, 8192], P('col', 'row')
- grad_gate_weight: float32 [8192, 14336], P('row', 'col')
- grad_up_weight: float32 [8192, 14336], P('row', 'col')
- grad_down_weight: float32 [8192, 14336], P('row', 'col')
The draws below stay inside these ranges and needn't reach their ends.
All inputs are finite; a program needn't handle non-finite values.
Results may differ from the reference program's by a relative error of at most 0.0049.
Values may be sent and summed in bfloat16 or wider, within the bound.
No kernel may reach another device: no remote copies, remote signals or barrier semaphores. Data moves between devices by JAX's collectives and lax.ppermute only.
A program may use at most 128 MiB of HBM per device.

```python
import jax
import jax.numpy as jnp
from jax import lax

D = 8192
FF = 14336
TOKENS = 2048


def raised(result, key, source, target, blocks, factor):
    def block_of(dim):
        return (jnp.arange(result.shape[dim]) // (result.shape[dim] // blocks)).reshape((-1,) + (1,) * (result.ndim - 1 - dim))

    near = jax.random.permutation(key, blocks)[block_of(target)]
    second = (block_of(target) + blocks // 2) % blocks
    return jnp.where((block_of(source) == near) | (block_of(source) == second), factor * result, result)


def block_scale(own_key, shape, pieces, low, high):
    def one(dim, parts):
        draws = jax.random.uniform(jax.random.fold_in(jax.random.fold_in(own_key, 6), dim), (parts,), jnp.float32, low / len(pieces), high / len(pieces))
        return jnp.repeat(jnp.exp(draws), shape[dim] // parts).reshape((-1,) + (1,) * (len(shape) - dim - 1))

    level = one(*pieces[0])
    for cut in pieces[1:]:
        level = level * one(*cut)
    return level


def noise(key, shape, scale, bound, split=(), kind=jnp.bfloat16):
    result = scale * jax.random.normal(key, shape, jnp.float32)
    if split:
        result = result * block_scale(key, shape, split, -0.22, 0.18)
    return jnp.clip(result, -bound, bound).astype(kind)


def bell_draw_with(rng, shape, scale, most, shards, heavy, held_as=jnp.bfloat16):
    array = scale * jax.random.normal(rng, shape, jnp.float32)
    if shards:
        array = array * block_scale(rng, shape, shards, -0.22, 0.18)
    return jnp.clip(raised(array, jax.random.fold_in(rng, 3), *heavy), -most, most).astype(held_as)


def setup_inputs(seed: int = 0) -> dict:
    splits = jax.random.split(jax.random.key(seed), 8)
    tokens = noise(splits[0], (TOKENS, D), 1.0, 6.0, ((0, 16), (1, 16)))
    grad_out = bell_draw_with(splits[1], (TOKENS, D), 0.25, 2.0, ((0, 16), (1, 16)), (1, 0, 16, 2.0))
    gate = noise(splits[2], (TOKENS, FF), 1.0, 6.0, ((0, 16), (1, 16)))
    up = noise(splits[3], (TOKENS, FF), 1.0, 6.0, ((0, 16), (1, 16)))
    gate_weight = noise(splits[4], (D, FF), D ** -0.5, 0.0625, ((0, 16), (1, 16)))
    up_weight = noise(splits[5], (D, FF), D ** -0.5, 0.0625, ((0, 16), (1, 16)))
    down_weight = noise(splits[6], (D, FF), FF ** -0.5, 0.046875, ((0, 16), (1, 16)))
    return {"tokens": tokens, "grad_out": grad_out, "gate": gate, "up": up, "gate_weight": gate_weight, "up_weight": up_weight, "down_weight": down_weight}


def reference(tokens, grad_out, gate, up, gate_weight, up_weight, down_weight):
    gate32 = gate.astype(jnp.float32)
    up32 = up.astype(jnp.float32)
    sigma = jax.nn.sigmoid(gate32)
    active = gate32 * sigma
    hidden = (active * up32).astype(jnp.bfloat16)
    grad_hidden = jnp.dot(grad_out, down_weight, preferred_element_type=jnp.float32)
    grad_up = (grad_hidden * active).astype(jnp.bfloat16)
    grad_gate = (grad_hidden * up32 * sigma * (1.0 + gate32 * (1.0 - sigma))).astype(jnp.bfloat16)
    grad_down_weight = jnp.dot(grad_out.T, hidden, preferred_element_type=jnp.float32)
    grad_gate_weight = jnp.dot(tokens.T, grad_gate, preferred_element_type=jnp.float32)
    grad_up_weight = jnp.dot(tokens.T, grad_up, preferred_element_type=jnp.float32)
    dims = (((1,), (1,)), ((), ()))
    grad_tokens = lax.dot_general(grad_gate, gate_weight, dims, preferred_element_type=jnp.float32)
    grad_tokens = grad_tokens + lax.dot_general(grad_up, up_weight, dims, preferred_element_type=jnp.float32)
    return grad_tokens.astype(jnp.bfloat16), grad_gate_weight, grad_up_weight, grad_down_weight
```

```python
import jax
import jax.numpy as jnp
from jax import lax
from jax.experimental import pallas as pl
from jax.experimental.pallas import tpu as pltpu
from jax.sharding import Mesh
from jax.sharding import PartitionSpec as P


ROW = ("x", "zh")
COL = ("y", "zl", "c")
NEAR = ("y", "zl")
STEPS = (0, -1, 1, 2)

BF16 = jnp.bfloat16
F32 = jnp.float32


def pull(block, axis, step):
    size = lax.axis_size(axis)
    return lax.ppermute(block, axis, [((i + step) % size, i) for i in range(size)])


def exchange(blocks, axes):
    return lax.all_to_all(blocks, axes, split_axis=0, concat_axis=0, tiled=True)


def spread(block, axes, size):
    return exchange(jnp.broadcast_to(block, (size, *block.shape)), axes)


def put(buffer, block, index):
    return lax.dynamic_update_slice_in_dim(buffer, block[None], index, axis=0)


def copied(sources, moves, shape):
    numbers = jnp.stack([jnp.int32(n) for _, at, to in moves for n in (at, to[0])])

    def body(numbers_ref, *refs):
        target, sems = refs[-2], refs[-1]
        copies = [
            pltpu.make_async_copy(
                refs[k].at[numbers_ref[2 * n]],
                target.at[(numbers_ref[2 * n + 1], *to[1:])],
                sems.at[n],
            )
            for n, (k, _, to) in enumerate(moves)
        ]
        for copy in copies:
            copy.start()
        for copy in copies:
            copy.wait()

    size = 1
    for n in shape:
        size *= n
    return pl.pallas_call(
        body,
        out_shape=jax.ShapeDtypeStruct(shape, sources[0].dtype),
        in_specs=[pl.BlockSpec(memory_space=pltpu.SMEM)]
        + [pl.BlockSpec(memory_space=pltpu.HBM)] * len(sources),
        out_specs=pl.BlockSpec(memory_space=pltpu.VMEM),
        scratch_shapes=[pltpu.SemaphoreType.DMA((len(moves),))],
        cost_estimate=pl.CostEstimate(
            flops=2_000_000, transcendentals=0, bytes_accessed=4 * size
        ),
    )(numbers, *sources)


def merged(early, kept, received, slots):
    def body(slots_ref, *refs):
        for k in range(3):
            refs[5][slots_ref[k]] = refs[k][...]
        refs[5][slots_ref[3]] = (refs[3][...] + refs[4][...]).astype(BF16)

    return pl.pallas_call(
        body,
        out_shape=jax.ShapeDtypeStruct((4, *kept.shape), BF16),
        in_specs=[pl.BlockSpec(memory_space=pltpu.SMEM)]
        + [pl.BlockSpec(memory_space=pltpu.VMEM)] * 5,
        out_specs=pl.BlockSpec(memory_space=pltpu.VMEM),
        cost_estimate=pl.CostEstimate(
            flops=2_000_000, transcendentals=0, bytes_accessed=20 * kept.size
        ),
        name="merged",
    )(jnp.stack(slots).astype(jnp.int32), *early, kept, received)


def ring_blocks(block, axis):
    left = pull(block, axis, -1)
    right = pull(block, axis, 1)
    half = block.shape[0] // 2
    far_low = pull(left[:half], axis, -1)
    far_high = pull(right[half:], axis, 1)
    return left, right, far_low, far_high


def ring_pairs(first, second, axis):
    lefts = [pull(v, axis, -1) for v in (first, second)]
    rights = [pull(v, axis, 1) for v in (first, second)]
    far = [pull(lefts[0], axis, -1), pull(rights[1], axis, 1)]
    return [[v, l, r, f] for v, l, r, f in zip((first, second), lefts, rights, far)]


def both_lows(block):
    zl = lax.axis_index("zl")
    other = pull(block, "zl", 1)
    return put(put(jnp.zeros((2, *block.shape), block.dtype), block, zl), other, 1 - zl)


def quarter(array, index, dim):
    return lax.dynamic_index_in_dim(array, index, axis=dim, keepdims=False)


def elementwise(grad_hidden, gate, up):
    gate32 = gate.astype(F32)
    up32 = up.astype(F32)
    grad32 = grad_hidden.astype(F32)
    sigma = jax.nn.sigmoid(gate32)
    active = gate32 * sigma
    grad_up = (grad32 * active).astype(BF16)
    grad_gate = (grad32 * up32 * sigma * (1.0 + gate32 * (1.0 - sigma))).astype(BF16)
    return grad_gate, grad_up


def hidden_of(gate, up):
    gate32 = gate.astype(F32)
    return (gate32 * jax.nn.sigmoid(gate32) * up.astype(F32)).astype(BF16)


def backward(tokens, grad_out, gate, up, gate_weight, up_weight, down_weight):
    x = lax.axis_index("x")
    zh = lax.axis_index("zh")
    c = lax.axis_index("c")
    rows, width = tokens.shape
    units = gate.shape[1]
    places = [(x + s) % 4 for s in STEPS]
    inner = (((1,), (1,)), ((), ()))
    outer = (((0,), (0,)), ((), ()))

    out_own = spread(both_lows(grad_out), "y", 4)
    own = exchange(out_own.reshape(4, 2 * rows, width), "x")
    own = jnp.concatenate([quarter(own, p, 0) for p in places], axis=1)
    grad_quarter = jnp.concatenate([own, pull(own, "c", 1)], axis=0)
    partial, at = None, 0
    for weight in (down_weight, *ring_blocks(down_weight, "x")):
        term = jnp.dot(
            grad_quarter[:, at : at + weight.shape[0]], weight, preferred_element_type=F32
        )
        at += weight.shape[0]
        partial = term if partial is None else partial + term
    partial = partial.astype(BF16)
    arrived = exchange(partial.reshape(4, rows, units), "zh")
    grad_hidden = arrived.astype(F32).sum(axis=0).astype(BF16)
    grad_hidden = spread(grad_hidden, "zh", 4)

    def slot(step):
        at = (zh + step) % 4
        return ((at % 2) ^ c) * 2 + at // 2

    def quarter_of(blocks):
        moves = [(k, 0, (slot(s),)) for k, s in enumerate(STEPS)]
        return copied([b[None] for b in blocks], moves, (4, rows, units))

    gates, ups = ring_pairs(gate, up, "zh")
    gates, ups = ring_pairs(quarter_of(gates), quarter_of(ups), "x")
    left, right, far_low, far_high = ring_blocks(grad_hidden, "x")
    grads = [grad_hidden, left, right, jnp.concatenate([far_low, far_high], axis=0)]

    def ordered(own):
        own = own.reshape(4, 2 * rows, width)
        moves = [(k, p, (2 * n + k,)) for n, p in enumerate(places) for k in range(2)]
        other = pull(own, "c", 1)
        return copied([own, other], moves, (8, 2 * rows, width)).reshape(-1, width)

    out_all = ordered(out_own)
    tokens_all = ordered(spread(both_lows(tokens), "y", 4))

    grads_gate, grads_up, hiddens, sums = [], [], [], []
    for i in range(4):
        ahead = lax.optimization_barrier((gates[i], ups[i]))
        hiddens.append(hidden_of(*ahead).reshape(4 * rows, units))
        grad_gate, grad_up = elementwise(grads[i], gates[i], ups[i])
        grad_gate = grad_gate.reshape(4 * rows, units)
        grad_up = grad_up.reshape(4 * rows, units)
        first = lax.dot_general(grad_gate, gate_weight, inner, preferred_element_type=F32)
        total = first + lax.dot_general(
            grad_up, up_weight, inner, preferred_element_type=F32
        )
        grads_gate.append(grad_gate)
        grads_up.append(grad_up)
        kept = total[: 2 * rows]
        received = pull(total[2 * rows :], "c", 1)
        if i < 3:
            sums.append((kept + received).astype(BF16))

    near = merged(sums, kept, received, places).reshape(8, rows, width)
    near = exchange(near, NEAR)
    result = near.astype(F32).sum(axis=0).astype(BF16)

    grad_down_weight = lax.dot_general(
        out_all, jnp.concatenate(hiddens, axis=0), outer, preferred_element_type=F32
    )

    def weight_grad(blocks):
        split = 12 * rows
        early = lax.dot_general(
            tokens_all[:split],
            jnp.concatenate(blocks[:3], axis=0),
            outer,
            preferred_element_type=F32,
        )
        return early + lax.dot_general(
            tokens_all[split:], blocks[3], outer, preferred_element_type=F32
        )

    grad_gate_weight = weight_grad(grads_gate)
    grad_up_weight = weight_grad(grads_up)
    return (result, grad_gate_weight, grad_up_weight, grad_down_weight)


def solution(mesh):
    finer = Mesh(mesh.devices.reshape(4, 4, 4, 2, 2), ("x", "zh", "y", "zl", "c"))
    return jax.shard_map(
        backward,
        mesh=finer,
        in_specs=(P(COL, ROW), P(COL, ROW)) + (P(ROW, COL),) * 5,
        out_specs=(P(COL, ROW), P(ROW, COL), P(ROW, COL), P(ROW, COL)),
        check_vma=False,
    )
```

```python
import jax
import jax.numpy as jnp
from jax import lax
from jax.experimental import pallas as pl
from jax.experimental.pallas import tpu as pltpu
from jax.sharding import Mesh
from jax.sharding import PartitionSpec as P


ROW = ("x", "zh")
COL = ("y", "zl", "c")
NEAR = ("y", "zl")
STEPS = (0, -1, 1, 2)

BF16 = jnp.bfloat16
F32 = jnp.float32


def pull(block, axis, step):
    size = lax.axis_size(axis)
    return lax.ppermute(block, axis, [((i + step) % size, i) for i in range(size)])


def exchange(blocks, axes):
    return lax.all_to_all(blocks, axes, split_axis=0, concat_axis=0, tiled=True)


def spread(block, axes, size):
    return exchange(jnp.broadcast_to(block, (size, *block.shape)), axes)


def put(buffer, block, index):
    return lax.dynamic_update_slice_in_dim(buffer, block[None], index, axis=0)


def copied(sources, moves, shape, outputs=1):
    numbers = jnp.stack([jnp.int32(n) for _, at, to, _ in moves for n in (at, to)])

    def body(numbers_ref, *refs):
        targets, sems = refs[len(sources) : -1], refs[-1]
        copies = [
            pltpu.make_async_copy(
                refs[k].at[numbers_ref[2 * n]],
                targets[t].at[numbers_ref[2 * n + 1]],
                sems.at[n],
            )
            for n, (k, _, _, t) in enumerate(moves)
        ]
        for copy in copies:
            copy.start()
        for copy in copies:
            copy.wait()

    size = outputs
    for n in shape:
        size *= n
    return pl.pallas_call(
        body,
        out_shape=[jax.ShapeDtypeStruct(shape, sources[0].dtype)] * outputs,
        in_specs=[pl.BlockSpec(memory_space=pltpu.SMEM)]
        + [pl.BlockSpec(memory_space=pltpu.HBM)] * len(sources),
        out_specs=[pl.BlockSpec(memory_space=pltpu.VMEM)] * outputs,
        scratch_shapes=[pltpu.SemaphoreType.DMA((len(moves),))],
        cost_estimate=pl.CostEstimate(
            flops=2_000_000, transcendentals=0, bytes_accessed=4 * size
        ),
    )(numbers, *sources)


def merged(totals, received, slots):
    rows, width = totals[0].shape[0] // 2, totals[0].shape[1]

    def body(slots_ref, *refs):
        for k in range(4):
            refs[8][slots_ref[k]] = (refs[k][...] + refs[4 + k][...]).astype(BF16)

    first = pl.BlockSpec((rows, width), lambda i: (0, 0))
    second = pl.BlockSpec((rows, width), lambda i: (1, 0))
    return pl.pallas_call(
        body,
        grid=(1,),
        out_shape=jax.ShapeDtypeStruct((4, rows, width), BF16),
        in_specs=[pl.BlockSpec(memory_space=pltpu.SMEM)] + [first] * 4 + [second] * 4,
        out_specs=pl.BlockSpec((4, rows, width), lambda i: (0, 0, 0)),
        cost_estimate=pl.CostEstimate(
            flops=2_000_000, transcendentals=0, bytes_accessed=40 * rows * width
        ),
        name="merged",
    )(jnp.stack(slots).astype(jnp.int32), *totals, *received)


def ring_blocks(block, axis):
    left = pull(block, axis, -1)
    right = pull(block, axis, 1)
    half = block.shape[0] // 2
    far_low = pull(left[:half], axis, -1)
    far_high = pull(right[half:], axis, 1)
    return left, right, far_low, far_high


def ring_pairs(first, second, axis):
    lefts = [pull(v, axis, -1) for v in (first, second)]
    rights = [pull(v, axis, 1) for v in (first, second)]
    far = [pull(lefts[0], axis, -1), pull(rights[1], axis, 1)]
    return [[v, l, r, f] for v, l, r, f in zip((first, second), lefts, rights, far)]


def both_lows(block):
    zl = lax.axis_index("zl")
    other = pull(block, "zl", 1)
    return put(put(jnp.zeros((2, *block.shape), block.dtype), block, zl), other, 1 - zl)


def quarter(array, index, dim):
    return lax.dynamic_index_in_dim(array, index, axis=dim, keepdims=False)


def prepared(gate, up):
    blocks, rows, units = gate.shape
    chunk = 16

    def body(gate_ref, up_ref, hidden_ref, active_ref, slope_ref):
        @pl.loop(0, rows // chunk)
        def _(n):
            at = pl.ds(pl.multiple_of(n * chunk, chunk), chunk)
            gate32 = gate_ref[0, at, :].astype(F32)
            up32 = up_ref[0, at, :].astype(F32)
            sigma = jax.nn.sigmoid(gate32)
            active = gate32 * sigma
            hidden_ref[0, at, :] = (active * up32).astype(BF16)
            active_ref[0, at, :] = active
            slope_ref[0, at, :] = up32 * sigma * (1.0 + gate32 * (1.0 - sigma))

    whole = pl.BlockSpec((1, rows, units), lambda i: (i, 0, 0))
    return pl.pallas_call(
        body,
        grid=(blocks,),
        out_shape=[jax.ShapeDtypeStruct(gate.shape, t) for t in (BF16, F32, F32)],
        in_specs=[whole] * 2,
        out_specs=[whole] * 3,
        cost_estimate=pl.CostEstimate(
            flops=20 * gate.size, transcendentals=gate.size, bytes_accessed=14 * gate.size
        ),
    )(gate, up)


def backward(tokens, grad_out, gate, up, gate_weight, up_weight, down_weight):
    x = lax.axis_index("x")
    zh = lax.axis_index("zh")
    c = lax.axis_index("c")
    rows, width = tokens.shape
    units = gate.shape[1]
    places = [(x + s) % 4 for s in STEPS]
    inner = (((1,), (1,)), ((), ()))
    outer = (((0,), (0,)), ((), ()))

    out_own = spread(both_lows(grad_out), "y", 4)
    own = exchange(out_own.reshape(4, 2 * rows, width), "x")
    own = jnp.concatenate([quarter(own, p, 0) for p in places], axis=1)
    grad_quarter = jnp.concatenate([own, pull(own, "c", 1)], axis=0)
    partial, at = None, 0
    for weight in (down_weight, *ring_blocks(down_weight, "x")):
        term = jnp.dot(
            grad_quarter[:, at : at + weight.shape[0]], weight, preferred_element_type=F32
        )
        at += weight.shape[0]
        partial = term if partial is None else partial + term
    partial = partial.astype(BF16)
    arrived = exchange(partial.reshape(4, rows, units), "zh")
    grad_hidden = arrived.astype(F32).sum(axis=0).astype(BF16)
    grad_hidden = spread(grad_hidden, "zh", 4)

    def slot(step):
        at = (zh + step) % 4
        return ((at % 2) ^ c) * 2 + at // 2

    gates, ups = ring_pairs(gate, up, "zh")
    moves = [(4 * t + k, 0, slot(s), t) for t in range(2) for k, s in enumerate(STEPS)]
    gates, ups = copied([b[None] for b in (*gates, *ups)], moves, (4, rows, units), outputs=2)
    gates, ups = ring_pairs(gates, ups, "x")
    left, right, far_low, far_high = ring_blocks(grad_hidden, "x")
    grads = [(grad_hidden,), (left,), (right,), (far_low, far_high)]

    def ordered(own):
        own = own.reshape(4, 2 * rows, width)
        moves = [(k, p, 2 * n + k, 0) for n, p in enumerate(places) for k in range(2)]
        other = pull(own, "c", 1)
        return copied([own, other], moves, (8, 2 * rows, width))[0].reshape(-1, width)

    out_all = ordered(out_own)
    tokens_all = ordered(spread(both_lows(tokens), "y", 4))

    grads_gate, grads_up, hiddens, totals, received = [], [], [], [], []
    for i in range(4):
        hidden, active, slope = prepared(gates[i], ups[i])
        hiddens.append(hidden.reshape(4 * rows, units))
        grad32 = jnp.concatenate(grads[i], axis=0).astype(F32)
        grad_gate = (grad32 * slope).astype(BF16).reshape(4 * rows, units)
        grad_up = (grad32 * active).astype(BF16).reshape(4 * rows, units)
        first = lax.dot_general(grad_gate, gate_weight, inner, preferred_element_type=F32)
        total = first + lax.dot_general(
            grad_up, up_weight, inner, preferred_element_type=F32
        )
        grads_gate.append(grad_gate)
        grads_up.append(grad_up)
        totals.append(total)
        received.append(pull(total, "c", 1))

    near = merged(totals, received, places).reshape(8, rows, width)
    near = exchange(near, NEAR)
    result = near.astype(F32).sum(axis=0).astype(BF16)

    def weight_grad(side, blocks):
        return lax.dot_general(
            side, jnp.concatenate(blocks, axis=0), outer, preferred_element_type=F32
        )

    grad_down_weight = weight_grad(out_all, hiddens)
    grad_gate_weight = weight_grad(tokens_all, grads_gate)
    grad_up_weight = weight_grad(tokens_all, grads_up)
    return (result, grad_gate_weight, grad_up_weight, grad_down_weight)


def solution(mesh):
    finer = Mesh(mesh.devices.reshape(4, 4, 4, 2, 2), ("x", "zh", "y", "zl", "c"))
    return jax.shard_map(
        backward,
        mesh=finer,
        in_specs=(P(COL, ROW), P(COL, ROW)) + (P(ROW, COL),) * 5,
        out_specs=(P(COL, ROW), P(ROW, COL), P(ROW, COL), P(ROW, COL)),
        check_vma=False,
    )
```
